32 devices in a mesh: dp: 8 (over z, x), mp: 4 (over y, core).
Axes of the slice: x: 2, y: 2, z: 4, core: 2. Of those that a mesh axis runs over, the one named last changes fastest.
Arguments:
- hidden: bfloat16 [2304, 5376], P('dp', 'mp'), may hold values from -6 to 6
- master: float32 [5376, 4096], P(('mp', 'dp')), may hold values from -0.078125 to 0.078125
- grad: float32 [5376, 4096], P(('mp', 'dp')), may hold values from -1500 to 1500, as said below
- row_factor: float32 [5376], P(('mp', 'dp')), may hold values from 0.01 to 1, as said below
- col_factor: float32 [4096], replicated, may hold values from 0.05 to 0.5
Outputs:
- ffn_out: bfloat16 [2304, 4096], P('dp', 'mp')
- update: float32 [5376, 4096], P(('mp', 'dp'))
- row_new: float32 [5376], P(('mp', 'dp'))
- col_new: float32 [4096], replicated
The draws below stay inside these ranges and needn't reach their ends.
Inputs may be any that keep to these rules, and one draw needn't show every extreme that they name: `grad`: every entry is finite. `row_factor`: every entry is positive.
All inputs are finite; a program needn't handle non-finite values.
Results may differ from the reference program's by a relative error of at most 0.0049.
Values may be sent and summed in bfloat16 or wider, within the bound.
No kernel may reach another device: no remote copies, remote signals or barrier semaphores. Data moves between devices by JAX's collectives and lax.ppermute only.
A program may use at most 64 MiB of HBM per device.

```python
import math
import jax
import jax.numpy as jnp
from jax import lax

D = 4096
FFW = 5376
STEP = 10
TOKENS = 2304
N_DP = 8
N_MP = 4


def draw_grad(key, part):
    key_base = jax.random.fold_in(key, 101)
    key_rows = jax.random.fold_in(key, 102)
    key_cols = jax.random.fold_in(key, 103)
    key_perm = jax.random.fold_in(key, 104)
    base = jnp.clip(jax.random.normal(key_base, (FFW, D), jnp.float32), -6.0, 6.0)
    low = jnp.log(0.3)
    high = jnp.log(3.0)
    row_scale = jnp.exp(jax.random.uniform(key_rows, (FFW, 1), jnp.float32, low, high))
    ramp = jnp.sqrt(1.0 + 2.0 * jnp.arange(FFW, dtype=jnp.float32)[:, None] / (FFW - 1))
    col_scale = jnp.exp(jax.random.uniform(key_cols, (1, D), jnp.float32, low, high))
    blocks = N_DP * N_MP
    group = FFW // blocks
    order = jax.random.permutation(key_perm, blocks)
    owner = order[jnp.arange(FFW) // group]
    marked = jnp.arange(D)[None, :] % blocks == owner[:, None]
    spike = jnp.where(marked, 30.0, 1.0)
    return (0.5 * base * row_scale * ramp * col_scale * spike).astype(jnp.float32)


def draw_row_factor(key, part):
    key_rough = jax.random.fold_in(key, 201)
    rough = jnp.exp(jax.random.uniform(key_rough, (FFW,), jnp.float32, jnp.log(0.1), 0.0))
    ramp = jnp.exp(-jnp.log(9.0) * jnp.arange(FFW, dtype=jnp.float32) / (FFW - 1))
    return (rough * ramp).astype(jnp.float32)


def block_scale(own_key, dims, cuts, smallest, top_value):
    def one(dim, shards_of):
        draws = jax.random.uniform(jax.random.fold_in(jax.random.fold_in(own_key, 6), dim), (shards_of,), jnp.float32, smallest / len(cuts), top_value / len(cuts))
        return jnp.repeat(jnp.exp(draws), dims[dim] // shards_of).reshape((-1,) + (1,) * (len(dims) - dim - 1))

    loudness = one(*cuts[0])
    for cut in cuts[1:]:
        loudness = loudness * one(*cut)
    return loudness


def gaussian(key, shape, spread, limit, split=(), held_as=jnp.bfloat16):
    result = spread * jax.random.normal(key, shape, jnp.float32)
    if split:
        result = result * block_scale(key, shape, split, -0.22, 0.18)
    return jnp.clip(result, -limit, limit).astype(held_as)


def setup_inputs(seed: int = 0) -> dict:
    streams_of = jax.random.split(jax.random.key(seed), 6)
    return {
        "hidden": gaussian(streams_of[0], (TOKENS, FFW), 1.0, 6.0, ((0, 8), (1, 4))),
        "master": gaussian(streams_of[1], (FFW, D), FFW ** -0.5, 0.078125, ((0, 32),), jnp.float32),
        "grad": draw_grad(jax.random.fold_in(streams_of[5], 71), 0),
        "row_factor": draw_row_factor(jax.random.fold_in(streams_of[5], 71), 0),
        "col_factor": jnp.clip(jnp.exp(jax.random.uniform(streams_of[4], (D,), jnp.float32, math.log(0.05), math.log(0.5))), 0.05, 0.5),
    }


def reference(hidden, master, grad, row_factor, col_factor):
    keep = 1.0 - STEP ** (-0.8)
    step_rate = min(0.01, STEP ** (-0.5))
    squared = grad * grad + 1e-30
    row_new = keep * row_factor + (1.0 - keep) * lax.optimization_barrier(jnp.mean(squared, axis=1))
    col_new = keep * col_factor + (1.0 - keep) * lax.optimization_barrier(jnp.mean(squared, axis=0))
    scaled = grad * lax.rsqrt(row_new[:, None] * col_new[None, :])
    root_mean = jnp.sqrt(jnp.mean(scaled * scaled))
    update = scaled / jnp.maximum(1.0, root_mean)
    weight = (master - step_rate * update).astype(jnp.bfloat16)
    ffn_out = jnp.dot(hidden, weight, preferred_element_type=jnp.float32).astype(jnp.bfloat16)
    return (ffn_out, update, row_new, col_new)
```

```python
import jax
import jax.numpy as jnp
from jax import lax
from jax.sharding import PartitionSpec as P

STEP = 10
CHUNKS = 4


def swap(value, axis, size, bit):
    return lax.ppermute(value, axis, [(i, i ^ bit) for i in range(size)])


def xor_sum(value, axis, size):
    terms = [value] + [swap(value, axis, size, s) for s in range(1, size)]
    while len(terms) > 1:
        terms = [terms[k] + terms[k + 1] for k in range(0, len(terms), 2)]
    return terms[0]


def matmul(a, b):
    return jnp.dot(a, b, preferred_element_type=jnp.float32)


def general_product(hidden, weight):
    partial_out = matmul(hidden, lax.all_gather(weight, "dp", axis=0, tiled=True))
    return lax.psum_scatter(partial_out, "mp", scatter_dimension=1, tiled=True).astype(jnp.bfloat16)


def exchanged_hidden(hidden, rows, n_dp):
    half = n_dp // 2
    me = lax.axis_index("dp")
    tokens = hidden.shape[0]
    blocks = jnp.transpose(hidden.reshape(tokens, n_dp, rows), (1, 0, 2))
    pick = lambda s: lax.dynamic_index_in_dim(blocks, me ^ s, 0, keepdims=False)
    theirs = swap(jnp.stack([pick(half + s) for s in range(half)]), "dp", n_dp, half)
    return [jnp.concatenate([pick(s), theirs[s]], axis=0) for s in range(half)]


def hybrid_product(tokens_by_block, weight_chunks, n_dp, n_mp):
    mp = lax.axis_index("mp")
    odd_core = (mp & 1) == 1
    odd_row = (mp & 2) == 2
    outs = []
    for own in weight_chunks:
        width = own.shape[1] // n_mp
        mid = own.shape[1] // 2
        tokens = tokens_by_block[0].shape[0] // 2
        from_x = swap(own, "dp", n_dp, 1)
        from_z = swap(own, "dp", n_dp, 2)
        far_left = swap(from_z[:, :mid], "dp", n_dp, 1)
        far_right = swap(from_x[:, mid:], "dp", n_dp, 2)
        h = tokens_by_block
        near = matmul(h[0], own) + matmul(h[1], from_x) + matmul(h[2], from_z)
        left = near[:, :mid] + matmul(h[3], far_left)
        right = near[:, mid:] + matmul(h[3], far_right)
        by_row = []
        sends = []
        for part in (left, right):
            even, odd = part[:, :width], part[:, width:]
            by_row.append(jnp.where(odd_core, odd, even))
            sends.append(jnp.where(odd_core, even, odd).astype(jnp.bfloat16))
        got = swap(jnp.stack(sends), "mp", n_mp, 1)
        low = by_row[0] + got[0].astype(jnp.float32)
        high = by_row[1] + got[1].astype(jnp.float32)
        kept = jnp.where(odd_row, high, low)
        sent = jnp.where(odd_row, low, high).astype(jnp.bfloat16)
        kept = kept + swap(sent, "mp", n_mp, 2).astype(jnp.float32)
        other = swap(kept[tokens:].astype(jnp.bfloat16), "dp", n_dp, n_dp // 2)
        outs.append((kept[:tokens] + other.astype(jnp.float32)).astype(jnp.bfloat16))
    return jnp.concatenate(outs, axis=1)


def make_body(n_dp, n_mp):
    hybrid = n_dp == 2**3 and n_mp == 2**2

    def body(hidden, master, grad, row_factor, col_factor):
        keep = 1.0 - STEP ** (-0.8)
        step_rate = min(0.01, STEP ** (-0.5))
        rows, features = grad.shape
        units = rows * n_dp * n_mp
        if hybrid:
            tokens_by_block = exchanged_hidden(hidden, rows, n_dp)
        squared = grad * grad + 1e-30
        row_new = keep * row_factor + (1.0 - keep) * jnp.mean(squared, axis=1)
        column_part = jnp.sum(squared, axis=0)
        weighted_part = jnp.sum(grad * grad / row_new[:, None], axis=0)
        if hybrid:
            stats = jnp.stack([column_part, weighted_part])
            stats = xor_sum(xor_sum(stats, "mp", n_mp), "dp", n_dp)
            column_total, weighted_total = stats[0], stats[1]
        else:
            column_total, weighted_total = lax.psum((column_part, weighted_part), ("dp", "mp"))
        col_new = keep * col_factor + (1.0 - keep) * column_total / float(units)
        square_total = jnp.sum(weighted_total / col_new)
        root_mean = jnp.sqrt(square_total / float(units * features))
        clip = jnp.maximum(1.0, root_mean)

        def update_of(g, c):
            return g * lax.rsqrt(row_new[:, None] * c[None, :]) / clip

        update = update_of(grad, col_new)
        if hybrid:
            owned = features // n_mp
            width = owned // CHUNKS
            chunks = []
            for c in range(CHUNKS):
                pick = lambda a: jnp.concatenate(
                    [a[..., m * owned + c * width : m * owned + (c + 1) * width] for m in range(n_mp)], axis=-1
                )
                chunks.append(pick((master - step_rate * update).astype(jnp.bfloat16)))
            ffn_out = hybrid_product(tokens_by_block, chunks, n_dp, n_mp)
        else:
            ffn_out = general_product(hidden, (master - step_rate * update).astype(jnp.bfloat16))
        return (ffn_out, update, row_new, col_new)

    return body


def solution(mesh):
    return jax.shard_map(
        make_body(mesh.shape["dp"], mesh.shape["mp"]),
        mesh=mesh,
        in_specs=(
            P("dp", "mp"),
            P(("mp", "dp"), None),
            P(("mp", "dp"), None),
            P(("mp", "dp")),
            P(),
        ),
        out_specs=(P("dp", "mp"), P(("mp", "dp"), None), P(("mp", "dp")), P()),
        check_vma=False,
    )
```
